32 devices in a mesh: dp: 8 (over y, x, core), mp: 4 (over z).
Axes of the slice: x: 2, y: 2, z: 4, core: 2. Of those that a mesh axis runs over, the one named last changes fastest.
Arguments:
- inputs: bfloat16 [1024, 6144], P('dp'), may hold values from -6 to 6
- pre_act: bfloat16 [1024, 12288], P('dp', 'mp'), may hold values from -6 to 6
- out_grad: bfloat16 [1024, 6144], P('dp'), may hold values from -6 to 6
- w_in: bfloat16 [6144, 12288], P(None, 'mp'), may hold values from -0.109375 to 0.109375
- w_out: bfloat16 [12288, 6144], P('mp'), may hold values from -0.0546875 to 0.0546875
- master_in: float32 [6144, 12288], P('dp', 'mp'), may hold values from -0.3 to 0.3
- master_out: float32 [12288, 6144], P('mp', 'dp'), may hold values from -0.3 to 0.3
- row_in: float32 [6144], P('dp'), may hold values from 12.8 to 686.08
- col_in: float32 [12288], P('mp'), may hold values from 25 to 128
- row_out: float32 [12288], P('mp'), may hold values from 25.6 to 1372.16
- col_out: float32 [6144], P('dp'), may hold values from 51 to 256
Outputs:
- input_grad: bfloat16 [1024, 6144], P('dp', 'mp')
- new_master_in: float32 [6144, 12288], P('dp', 'mp')
- new_master_out: float32 [12288, 6144], P('mp', 'dp')
The draws below stay inside these ranges and needn't reach their ends.
All inputs are finite; a program needn't handle non-finite values.
Results may differ from the reference program's by a relative error of at most 0.012.
Values may be sent and summed in bfloat16 or wider, within the bound.
No kernel may reach another device: no remote copies, remote signals or barrier semaphores. Data moves between devices by JAX's collectives and lax.ppermute only.
A program may use at most 256 MiB of HBM per device.

```python
import math
import jax
import jax.numpy as jnp
from jax import lax

D = 6144
FF = 12288
TOK_DEV = 128
TOKENS = 1024
N_DP = 8


def falling_factor(key, count, high, ratio):
    place = jnp.arange(count, dtype=jnp.float32) / float(count)
    noise = jax.random.uniform(key, (count,), jnp.float32, -0.28, 0.28)
    return high * jnp.exp(-jnp.log(ratio) * place + noise)


def draw_row_in(key, part):
    return falling_factor(jax.random.fold_in(key, 11), D, TOKENS * 0.5, 10.0)


def draw_row_out(key, part):
    return falling_factor(jax.random.fold_in(key, 23), FF, TOKENS * 1.0, 10.0)


def spiked(entries, key, source, target, blocks, factor):
    owner, partner = [(jnp.arange(entries.shape[position]) // (entries.shape[position] // blocks)).reshape([-1 if axis == position else 1 for axis in range(entries.ndim)]) for position in (source, target)]
    chosen = jax.random.permutation(key, blocks)[partner]
    strong = (owner == chosen) | (owner == (partner + blocks // 2) % blocks)
    return jnp.where(strong, factor * entries, entries)


def levels(rng, extent, cuts, least, high):
    loudness, own = 1.0, jax.random.fold_in(rng, 6)
    for position, blocks in cuts:
        heights = jnp.exp(jax.random.uniform(jax.random.fold_in(own, position), (blocks,), jnp.float32, least / len(cuts), high / len(cuts)))
        loudness = loudness * jnp.repeat(heights, extent[position] // blocks).reshape([-1 if axis == position else 1 for axis in range(len(extent))])
    return loudness


def scatter_about(stream_key, extent, width, most, shards=(), held_as=jnp.bfloat16):
    entries = width * jax.random.normal(stream_key, extent, jnp.float32)
    if shards:
        entries = entries * levels(stream_key, extent, shards, -0.22, 0.18)
    return jnp.clip(entries, -most, most).astype(held_as)


def noise_with(rng, dims, deviation, reach, cuts, heavy, held_as=jnp.bfloat16):
    drawn = deviation * jax.random.normal(rng, dims, jnp.float32)
    if cuts:
        drawn = drawn * levels(rng, dims, cuts, -0.22, 0.18)
    return jnp.clip(spiked(drawn, jax.random.fold_in(rng, 3), *heavy), -reach, reach).astype(held_as)


def setup_inputs(seed: int = 0) -> dict:
    keys = jax.random.split(jax.random.key(seed), 12)
    inputs = noise_with(keys[0], (TOKENS, D), 1.0, 6.0, ((0, 8),), (0, 1, 8, 2.0))
    pre_act = scatter_about(keys[1], (TOKENS, FF), 1.0, 6.0, ((0, 8), (1, 4)))
    out_grad = noise_with(keys[2], (TOKENS, D), 1.0, 6.0, ((0, 8),), (0, 1, 8, 2.0))
    w_in = noise_with(keys[3], (D, FF), D ** -0.5, 0.109375, ((1, 4),), (1, 0, 4, 2.0))
    w_out = scatter_about(keys[4], (FF, D), FF ** -0.5, 0.0546875, ((0, 4),))
    master_in = scatter_about(keys[5], (D, FF), 0.05, 0.3, ((0, 8), (1, 4)), jnp.float32)
    master_out = scatter_about(keys[6], (FF, D), 0.05, 0.3, ((0, 4), (1, 8)), jnp.float32)
    row_in = draw_row_in(jax.random.fold_in(keys[11], 71), 0)
    col_in = jnp.clip(jnp.exp(math.log(128.0) - 1.6331544 * jax.random.uniform(keys[8], (FF,), jnp.float32) ** levels(keys[8], (FF,), ((0, 4),), -0.2, 0.2)), 25.0, 128.0)
    row_out = draw_row_out(jax.random.fold_in(keys[11], 71), 0)
    col_out = jnp.clip(jnp.exp(math.log(256.0) - 1.6133518 * jax.random.uniform(keys[10], (D,), jnp.float32) ** levels(keys[10], (D,), ((0, 8),), -0.2, 0.2)), 51.0, 256.0)
    return dict(inputs=inputs, pre_act=pre_act, out_grad=out_grad, w_in=w_in, w_out=w_out, master_in=master_in, master_out=master_out, row_in=row_in, col_in=col_in, row_out=row_out, col_out=col_out)


decay_rate = 0.8
step_size = 0.05
tiny_square = 1e-30

def gelu_parts(pre):
    cumulative = 0.5 * (1.0 + jax.scipy.special.erf(pre * (1.0 / math.sqrt(2.0))))
    density = jnp.exp(-0.5 * pre * pre) * (1.0 / math.sqrt(2.0 * math.pi))
    return (pre * cumulative, cumulative + pre * density)

def adafactor(grad, master, row_state, col_state):
    square = grad * grad + tiny_square
    row_new = decay_rate * row_state + (1.0 - decay_rate) * lax.optimization_barrier(jnp.mean(square, axis=1))
    col_new = decay_rate * col_state + (1.0 - decay_rate) * lax.optimization_barrier(jnp.mean(square, axis=0))
    second = row_new[:, None] * col_new[None, :] / jnp.mean(row_new)
    update = grad / jnp.sqrt(second)
    return master - step_size * update

def reference(inputs, pre_act, out_grad, w_in, w_out, master_in, master_out, row_in, col_in, row_out, col_out):
    active, slope = gelu_parts(pre_act.astype(jnp.float32))
    hidden = active.astype(jnp.bfloat16)
    hid_grad = jnp.dot(out_grad, w_out.T, preferred_element_type=jnp.float32)
    pre_grad = (hid_grad * slope).astype(jnp.bfloat16)
    input_grad = jnp.dot(pre_grad, w_in.T, preferred_element_type=jnp.float32).astype(jnp.bfloat16)

    def group(totals, index):
        begin = (index * TOK_DEV).astype(jnp.int32)
        rows_x = lax.dynamic_slice_in_dim(inputs, begin, TOK_DEV, 0)
        rows_g = lax.dynamic_slice_in_dim(pre_grad, begin, TOK_DEV, 0)
        rows_h = lax.dynamic_slice_in_dim(hidden, begin, TOK_DEV, 0)
        rows_y = lax.dynamic_slice_in_dim(out_grad, begin, TOK_DEV, 0)
        part_in = jnp.dot(rows_x.T, rows_g, preferred_element_type=jnp.float32).astype(jnp.bfloat16)
        part_out = jnp.dot(rows_h.T, rows_y, preferred_element_type=jnp.float32).astype(jnp.bfloat16)
        part_in, part_out = lax.optimization_barrier((part_in, part_out))
        return ((totals[0] + part_in.astype(jnp.float32), totals[1] + part_out.astype(jnp.float32)), None)
    start_sums = (jnp.zeros((D, FF), jnp.float32), jnp.zeros((FF, D), jnp.float32))
    (grad_in, grad_out), _ = lax.scan(group, start_sums, jnp.arange(N_DP, dtype=jnp.int32))
    new_master_in = adafactor(grad_in, master_in, row_in, col_in)
    new_master_out = adafactor(grad_out, master_out, row_out, col_out)
    return (input_grad, new_master_in, new_master_out)
```

```python
import functools
import math

import jax
import jax.numpy as jnp
from jax import lax
from jax.experimental import pallas as pl
from jax.experimental.pallas import tpu as pltpu
from jax.sharding import PartitionSpec as P


decay_rate = 0.8
step_size = 0.05
tiny_square = 1e-30
LANES = 128
bf16 = jnp.bfloat16
f32 = jnp.float32
VMEM = pltpu.VMEM


def gelu_parts(pre):
    cumulative = 0.5 * (1.0 + lax.erf(pre * (1.0 / math.sqrt(2.0))))
    density = jnp.exp(-0.5 * pre * pre) * (1.0 / math.sqrt(2.0 * math.pi))
    return (pre * cumulative, cumulative + pre * density)


def dot(left, right, dims):
    return lax.dot_general(left, right, (dims, ((), ())), preferred_element_type=f32)


def params(limit_mb=48):
    return pltpu.CompilerParams(
        dimension_semantics=("arbitrary",), vmem_limit_bytes=limit_mb * 1024 * 1024
    )


def cost(flops, moved):
    return pl.CostEstimate(flops=int(flops), bytes_accessed=int(moved), transcendentals=0)


def pack_kernel(piece, place_ref, inputs_ref, grads_ref, pre_ref, x1, y1, c1, own):
    me, half = place_ref[0], place_ref[1]
    hp = piece // 2
    units = pre_ref.shape[1]

    def put(source, target, row, partner, first, rows):
        base = (me ^ partner) * piece + first
        for block in range(rows // LANES):
            columns = pl.ds(pl.multiple_of(base + block * LANES, LANES), LANES)
            target[row + block * LANES : row + (block + 1) * LANES, :] = source[:, columns]

    def halves(target, row, order):
        for k, (source, partner) in enumerate(order):
            put(source, target, row + k * hp, partner, half * hp, hp)

    i, g = inputs_ref, grads_ref
    halves(x1, 0, ((i, 2), (g, 2), (i, 3), (g, 3)))
    halves(x1, 4 * hp + units, ((i, 7), (i, 6)))
    halves(y1, 0, ((g, 6), (g, 7)))
    halves(y1, 2 * hp + units, ((i, 5), (g, 5), (i, 4), (g, 4)))
    put(i, c1, units, 1, 0, piece)
    put(g, c1, units + piece, 1, 0, piece)
    put(i, own, 0, 0, 0, piece)
    put(g, own, piece, 0, 0, piece)

    def gelu_block(block, _):
        columns = pl.ds(pl.multiple_of(block * LANES, LANES), LANES)
        active, _ = gelu_parts(pre_ref[:, columns].astype(f32))
        turned = active.T.astype(bf16)
        row = block * LANES
        x1[pl.ds(pl.multiple_of(4 * hp + row, LANES), LANES), :] = turned
        y1[pl.ds(pl.multiple_of(2 * hp + row, LANES), LANES), :] = turned
        c1[pl.ds(pl.multiple_of(row, LANES), LANES), :] = turned
        return 0

    lax.fori_loop(0, units // LANES, gelu_block, 0)


def pack(piece, place, inputs, grads, pre):
    units = pre.shape[1]
    rows = (3 * piece + units, 3 * piece + units, units + 2 * piece, 2 * piece)
    return pl.pallas_call(
        functools.partial(pack_kernel, piece),
        out_shape=[jax.ShapeDtypeStruct((r, LANES), bf16) for r in rows],
        in_specs=[pl.BlockSpec(memory_space=pltpu.SMEM)] + [pl.BlockSpec(memory_space=VMEM)] * 3,
        out_specs=[pl.BlockSpec(memory_space=VMEM)] * 4,
        compiler_params=pltpu.CompilerParams(vmem_limit_bytes=24 * 1024 * 1024),
        cost_estimate=cost(1e6, 9e6),
        name="pack",
    )(place, inputs, grads, pre)


def pre_grad_kernel(grads_ref, weight_ref, pre_ref, out_ref):
    product = dot(grads_ref[...], weight_ref[...], ((1,), (1,)))
    _, slope = gelu_parts(pre_ref[...].astype(f32))
    value = (product * slope).astype(bf16)
    for block in range(value.shape[1] // LANES):
        rows = slice(block * LANES, (block + 1) * LANES)
        out_ref[rows, :] = value[:, rows]


def pre_grad_blocks(grads, w_out, pre, step=256):
    units, width = w_out.shape
    tokens = grads.shape[0]
    return pl.pallas_call(
        pre_grad_kernel,
        grid=(units // step,),
        out_shape=jax.ShapeDtypeStruct((units, LANES), bf16),
        in_specs=[
            pl.BlockSpec((tokens, width), lambda n: (0, 0)),
            pl.BlockSpec((step, width), lambda n: (n, 0)),
            pl.BlockSpec((tokens, step), lambda n: (0, n)),
        ],
        out_specs=pl.BlockSpec((step, LANES), lambda n: (n, 0)),
        compiler_params=params(),
        cost_estimate=cost(2 * tokens * units * width, 2 * units * width),
        name="pre_grad",
    )(grads, w_out, pre)


def input_grad_kernel(_, grad_ref, weight_ref, out_ref, left):
    @pl.when((pl.program_id(0) == 0) & (pl.program_id(1) == 0))
    def _():
        for block in range(left.shape[1] // LANES):
            rows = slice(block * LANES, (block + 1) * LANES)
            left[:, rows] = grad_ref[rows, :]

    out_ref[...] = dot(left[...], weight_ref[...], ((1,), (1,))).astype(bf16)


def input_grad_parts(place, blocks, w_in, n_mp, step=512):
    width, units = w_in.shape
    part = width // n_mp
    per = part // step

    def weight_index(owner, n, place_ref):
        chunk = place_ref[0] ^ ((owner & 1) * 2 + (owner >> 1))
        return (chunk * per + n, 0)

    return pl.pallas_call(
        input_grad_kernel,
        grid_spec=pltpu.PrefetchScalarGridSpec(
            num_scalar_prefetch=1,
            grid=(n_mp, per),
            in_specs=[
                pl.BlockSpec((units, LANES), lambda o, n, p: (0, 0)),
                pl.BlockSpec((step, units), weight_index),
            ],
            out_specs=pl.BlockSpec((None, LANES, step), lambda o, n, p: (o, 0, n)),
            scratch_shapes=[pltpu.VMEM((LANES, units), bf16)],
        ),
        out_shape=jax.ShapeDtypeStruct((n_mp, LANES, part), bf16),
        compiler_params=pltpu.CompilerParams(
            dimension_semantics=("arbitrary", "arbitrary"), vmem_limit_bytes=48 * 1024 * 1024
        ),
        cost_estimate=cost(2 * LANES * units * width, 2 * units * width),
        name="input_grad",
    )(place, blocks, w_in)


def window(ref_rows, block_rows, index):
    return pl.BlockSpec((block_rows, LANES), index)


def fixed(rows, block):
    return pl.BlockSpec((rows, LANES), lambda n: (block, 0))


def moving(rows, first, low=0, high=None):
    def index(n):
        k = n - low
        if high is not None:
            k = jnp.clip(k, 0, high - low - 1)
        return (first + k, 0)

    return pl.BlockSpec((rows, LANES), index)


def spread(half, piece, refs, place, turn, target):
    hp = piece // 2
    for slot, (mine, other) in enumerate(refs):
        parts = ((mine, 0),) if other is None else ((mine, half * hp), (other, (1 - half) * hp))
        for ref, base in parts:
            for block in range(ref.shape[0] // LANES):
                value = ref[block * LANES : (block + 1) * LANES, :]
                at = base + block * LANES
                if not isinstance(at, int):
                    at = pl.multiple_of(at, LANES)
                tokens = slice(slot * LANES, (slot + 1) * LANES)
                if turn:
                    target[pl.ds(at, LANES), tokens] = value.astype(f32).T.astype(bf16)
                else:
                    target[tokens, pl.ds(at, LANES)] = value


def pair_up(refs):
    return [(refs[0], None), (refs[1], None)] + [(refs[k], refs[k + 1]) for k in range(2, 14, 2)]


def grad_out_kernel(piece, split, place_ref, *refs):
    hidden, pieces = refs[:10], refs[10:24]
    g_ref, rows_ref, cols_ref, right = refs[24:]
    n = pl.program_id(0)

    @pl.when(n == 0)
    def _():
        spread(place_ref[1], piece, pair_up(pieces), None, False, right)
        cols_ref[...] = jnp.zeros_like(cols_ref)

    first = n < split
    slots = [ref[...] for ref in hidden[:6]]
    slots += [
        jnp.where(first, hidden[6][...], hidden[7][...]),
        jnp.where(first, hidden[8][...], hidden[9][...]),
    ]
    left = jnp.concatenate(slots, axis=1)
    grad = dot(left, right[...], ((1,), (0,)))
    square = grad * grad + tiny_square
    g_ref[...] = grad.astype(bf16)
    ones = jnp.ones((8, piece), bf16)
    rows_ref[...] = dot(ones, square.astype(bf16), ((1,), (1,)))[:1]
    cols_ref[...] += jnp.sum(square, axis=0, keepdims=True)


def grad_out(piece, units, place, hidden, pieces):
    rows = piece // 2
    steps = units // rows
    return pl.pallas_call(
        functools.partial(grad_out_kernel, piece, steps // 2),
        grid=(steps,),
        out_shape=[
            jax.ShapeDtypeStruct((units, piece), bf16),
            jax.ShapeDtypeStruct((1, units), f32),
            jax.ShapeDtypeStruct((1, piece), f32),
        ],
        in_specs=[pl.BlockSpec(memory_space=pltpu.SMEM)]
        + [spec for _, spec in hidden]
        + [spec for _, spec in pieces],
        out_specs=[
            pl.BlockSpec((rows, piece), lambda n: (n, 0)),
            pl.BlockSpec((1, rows), lambda n: (0, n)),
            pl.BlockSpec((1, piece), lambda n: (0, 0)),
        ],
        scratch_shapes=[pltpu.VMEM((8 * LANES, piece), bf16)],
        compiler_params=params(),
        cost_estimate=cost(16 * LANES * units * piece, 16 * LANES * units + 2 * units * piece),
        name="grad_out",
    )(place, *[a for a, _ in hidden], *[a for a, _ in pieces])


def grad_in_kernel(piece, split, place_ref, *refs):
    slopes, pieces = refs[:10], refs[10:24]
    g_ref, rows_ref, cols_ref, left = refs[24:]
    n = pl.program_id(0)

    @pl.when(n == 0)
    def _():
        spread(place_ref[1], piece, pair_up(pieces), None, True, left)
        rows_ref[...] = jnp.zeros_like(rows_ref)

    first = n < split
    slots = [ref[...] for ref in slopes[:6]]
    slots += [
        jnp.where(first, slopes[6][...], slopes[7][...]),
        jnp.where(first, slopes[8][...], slopes[9][...]),
    ]
    count = slots[0].shape[0] // LANES
    right = jnp.concatenate(
        [
            jnp.concatenate([s[b * LANES : (b + 1) * LANES] for b in range(count)], axis=1)
            for s in slots
        ],
        axis=0,
    )
    grad = dot(left[...], right, ((1,), (0,)))
    square = grad * grad + tiny_square
    g_ref[...] = grad.astype(bf16)
    cols_ref[...] = jnp.sum(square, axis=0, keepdims=True)
    ones = jnp.ones((8, count * LANES), bf16)
    rows_ref[...] += dot(ones, square.astype(bf16), ((1,), (1,)))[:1]


def grad_in(piece, units, place, slopes, pieces):
    rows = piece
    steps = units // rows
    return pl.pallas_call(
        functools.partial(grad_in_kernel, piece, steps // 2),
        grid=(steps,),
        out_shape=[
            jax.ShapeDtypeStruct((piece, units), bf16),
            jax.ShapeDtypeStruct((1, piece), f32),
            jax.ShapeDtypeStruct((1, units), f32),
        ],
        in_specs=[pl.BlockSpec(memory_space=pltpu.SMEM)]
        + [spec for _, spec in slopes]
        + [spec for _, spec in pieces],
        out_specs=[
            pl.BlockSpec((piece, rows), lambda n: (0, n)),
            pl.BlockSpec((1, piece), lambda n: (0, 0)),
            pl.BlockSpec((1, rows), lambda n: (0, n)),
        ],
        scratch_shapes=[pltpu.VMEM((piece, 8 * LANES), bf16)],
        compiler_params=params(),
        cost_estimate=cost(16 * LANES * units * piece, 16 * LANES * units + 2 * units * piece),
        name="grad_in",
    )(place, *[a for a, _ in slopes], *[a for a, _ in pieces])


def swap(value, bit, axis, count):
    return lax.ppermute(value, axis, [(k, k ^ bit) for k in range(count)])


def butterfly(value, bits, axis, count):
    for bit in bits:
        value = value + swap(value, bit, axis, count)
    return value


def with_scalar(vector, scalar):
    return jnp.concatenate([vector, jnp.broadcast_to(scalar.reshape(1, 1), (1, LANES))], axis=1)


def apply_update(master, grad, rows, cols, mean):
    down = lax.rsqrt(rows) * (step_size * jnp.sqrt(mean))
    return master - grad.astype(f32) * down[:, None] * lax.rsqrt(cols)[None, :]


def fast_body(
    inputs, pre_act, out_grad, w_in, w_out, master_in, master_out, row_in, col_in, row_out, col_out
):
    n_dp, n_mp = 8, 4
    width, units = w_in.shape
    piece = width // n_dp
    hp = piece // 2
    me, z = lax.axis_index("dp"), lax.axis_index("mp")
    place = jnp.stack([me, z & 1]).astype(jnp.int32)
    dp = lambda value, bit: swap(value, bit, "dp", n_dp)
    mp = lambda value, bit: swap(value, bit, "mp", n_mp)

    x1, y1, c1, own = pack(piece, place, inputs, out_grad, pre_act)
    x1r, y1r, c1r = dp(x1, 2), dp(y1, 4), dp(c1, 1)
    pg = pre_grad_blocks(out_grad, w_out, pre_act)
    y2r = dp(x1r[4 * hp + units // 2 :], 4)
    x2r = dp(y1r[: 2 * hp + units // 2], 2)
    z1x = mp(x1r[: 4 * hp], 1)
    z1y = mp(y1r[2 * hp + units :], 1)
    c2x = dp(x1r[2 * hp : 4 * hp + units], 1)
    c2y = dp(y1r[2 * hp : 4 * hp + units], 1)
    z2y = mp(y2r[units // 2 :], 1)
    z2x = mp(x2r[: 2 * hp], 1)
    c3y = dp(y2r[: units // 2 + hp], 1)
    c3x = dp(x2r[hp:], 1)
    cz = dp(jnp.concatenate([z1x[2 * hp :], z1y[: 2 * hp], z2y[:hp], z2x[hp:]], axis=0), 1)

    ub, hb = units // hp, units // (2 * hp)
    hidden = [
        (c1, moving(hp, 0)),
        (c1r, moving(hp, 0)),
        (x1r, moving(hp, 4)),
        (c2x, moving(hp, 2)),
        (y1r, moving(hp, 2)),
        (c2y, moving(hp, 0)),
        (x2r, moving(hp, 2, 0, hb)),
        (y2r, moving(hp, 0, hb, ub)),
        (c3x, moving(hp, 1, 0, hb)),
        (c3y, moving(hp, 0, hb, ub)),
    ]
    whole = units // piece
    out_pieces = [
        (own, fixed(piece, 1)),
        (c1r, fixed(piece, whole + 1)),
        (x1r, fixed(hp, 1)),
        (z1x, fixed(hp, 1)),
        (c2x, fixed(hp, 1)),
        (cz, fixed(hp, 1)),
        (y1r, fixed(hp, ub + 5)),
        (z1y, fixed(hp, 3)),
        (c2y, fixed(hp, ub + 1)),
        (cz, fixed(hp, 3)),
        (x2r, fixed(hp, 0)),
        (z2x, fixed(hp, 0)),
        (c3x, fixed(hp, 0)),
        (cz, fixed(hp, 5)),
    ]
    in_pieces = [
        (own, fixed(piece, 0)),
        (c1r, fixed(piece, whole)),
        (x1r, fixed(hp, 0)),
        (z1x, fixed(hp, 0)),
        (c2x, fixed(hp, 0)),
        (cz, fixed(hp, 0)),
        (y1r, fixed(hp, ub + 4)),
        (z1y, fixed(hp, 2)),
        (c2y, fixed(hp, ub)),
        (cz, fixed(hp, 2)),
        (y2r, fixed(hp, hb + 1)),
        (z2y, fixed(hp, 1)),
        (c3y, fixed(hp, hb)),
        (cz, fixed(hp, 4)),
    ]

    px1, py1, pc1 = dp(pg, 2), dp(pg, 4), dp(pg, 1)
    py2, px2 = dp(px1[: units // 2], 4), dp(py1[units // 2 :], 2)
    pc2, pc4 = dp(px1, 1), dp(py1, 1)
    pc6a, pc6b = dp(py2, 1), dp(px2, 1)

    parts = input_grad_parts(z.astype(jnp.int32).reshape(1), pg, w_in, n_mp)
    near = mp(parts[2:], 1)
    held = parts[:2].astype(f32) + near.astype(f32)
    far = mp(held[1].astype(bf16), 2)
    input_grad = (held[0] + far.astype(f32)).astype(bf16)

    g_out, rows_o, cols_o = grad_out(piece, units, place, hidden, out_pieces)
    hidden_out = butterfly(rows_o, (1, 2, 4), "dp", n_dp)[0]
    rows_out = decay_rate * row_out + (1.0 - decay_rate) * hidden_out / width
    sums = butterfly(with_scalar(cols_o, jnp.sum(rows_out)), (1, 2), "mp", n_mp)[0]
    ff = units * n_mp
    cols_out = decay_rate * col_out + (1.0 - decay_rate) * sums[:piece] / ff
    new_master_out = apply_update(master_out, g_out, rows_out, cols_out, sums[piece] / ff)

    nb = units // (2 * piece)
    slopes = [
        (pg, moving(piece, 0)),
        (pc1, moving(piece, 0)),
        (px1, moving(piece, 0)),
        (pc2, moving(piece, 0)),
        (py1, moving(piece, 0)),
        (pc4, moving(piece, 0)),
        (py2, moving(piece, 0, 0, nb)),
        (px2, moving(piece, 0, nb, 2 * nb)),
        (pc6a, moving(piece, 0, 0, nb)),
        (pc6b, moving(piece, 0, nb, 2 * nb)),
    ]
    g_in, rows_i, cols_i = grad_in(piece, units, place, slopes, in_pieces)
    width_in = butterfly(rows_i, (1, 2), "mp", n_mp)[0]
    rows_in = decay_rate * row_in + (1.0 - decay_rate) * width_in / ff
    sums = butterfly(with_scalar(cols_i, jnp.sum(rows_in)), (1, 2, 4), "dp", n_dp)[0]
    cols_in = decay_rate * col_in + (1.0 - decay_rate) * sums[:units] / width
    new_master_in = apply_update(master_in, g_in, rows_in, cols_in, sums[units] / width)
    return (input_grad, new_master_in, new_master_out)


def plain_body(
    inputs, pre_act, out_grad, w_in, w_out, master_in, master_out, row_in, col_in, row_out, col_out
):
    width, units = w_in.shape
    active, slope = gelu_parts(pre_act.astype(f32))
    hidden = lax.all_gather(active.astype(bf16), "dp", axis=0, tiled=True)
    hid_grad = dot(out_grad, w_out, ((1,), (1,)))
    pre_grad = (hid_grad * slope).astype(bf16)
    input_grad = lax.psum_scatter(
        dot(w_in, pre_grad, ((1,), (1,))), "mp", scatter_dimension=0, tiled=True
    ).T.astype(bf16)
    every = lax.all_gather(pre_grad, "dp", axis=0, tiled=True)
    my_inputs = lax.all_to_all(inputs, "dp", 1, 0, tiled=True)
    my_grads = lax.all_to_all(out_grad, "dp", 1, 0, tiled=True)
    grad_in_all = dot(my_inputs, every, ((0,), (0,)))
    grad_out_all = dot(hidden, my_grads, ((0,), (0,)))
    square_in = grad_in_all * grad_in_all + tiny_square
    square_out = grad_out_all * grad_out_all + tiny_square
    width_in, width_out = lax.psum((jnp.sum(square_in, 1), jnp.sum(square_out, 0)), "mp")
    hidden_in, hidden_out = lax.psum((jnp.sum(square_in, 0), jnp.sum(square_out, 1)), "dp")
    ff = units * lax.axis_size("mp")
    rows_in = decay_rate * row_in + (1.0 - decay_rate) * width_in / ff
    cols_in = decay_rate * col_in + (1.0 - decay_rate) * hidden_in / width
    rows_out = decay_rate * row_out + (1.0 - decay_rate) * hidden_out / width
    cols_out = decay_rate * col_out + (1.0 - decay_rate) * width_out / ff
    mean_in = lax.psum(jnp.sum(rows_in), "dp") / width
    mean_out = lax.psum(jnp.sum(rows_out), "mp") / ff
    return (
        input_grad,
        apply_update(master_in, grad_in_all, rows_in, cols_in, mean_in),
        apply_update(master_out, grad_out_all, rows_out, cols_out, mean_out),
    )


def solution(mesh):
    in_specs = (
        P("dp", None),
        P("dp", "mp"),
        P("dp", None),
        P(None, "mp"),
        P("mp", None),
        P("dp", "mp"),
        P("mp", "dp"),
        P("dp"),
        P("mp"),
        P("mp"),
        P("dp"),
    )
    out_specs = (P("dp", "mp"), P("dp", "mp"), P("mp", "dp"))

    def body(*args):
        tokens, (width, units) = args[0].shape[0], args[3].shape
        fits = tokens == LANES and width % (16 * LANES) == 0 and width % (4 * 512) == 0
        fits = fits and units % (2 * (width // 8)) == 0 and units % 256 == 0
        fast = (mesh.shape["dp"], mesh.shape["mp"]) == (8, 4) and fits
        return (fast_body if fast else plain_body)(*args)

    return jax.shard_map(body, mesh=mesh, in_specs=in_specs, out_specs=out_specs, check_vma=False)
```
